64 devices in a mesh: dp: 8 (over x, y, core), tp: 8 (over z).
Axes of the slice: x: 2, y: 2, z: 8, core: 2. Of those that a mesh axis runs over, the one named last changes fastest.
The devices are a block of a 4x4x8 slice.
Arguments:
- x: bfloat16 [16384, 4096], P('dp'), parts along dimension 0
- dy: bfloat16 [16384, 4096], P('dp'), parts along dimension 0
- gate: bfloat16 [16384, 10240], P('dp', 'tp'), parts along dimension 0
- up: bfloat16 [16384, 10240], P('dp', 'tp'), parts along dimension 0
- w_gate: bfloat16 [4096, 10240], P(None, 'tp')
- w_up: bfloat16 [4096, 10240], P(None, 'tp')
- w_down: bfloat16 [10240, 4096], P('tp')
Outputs:
- output 1: bfloat16 [16384, 4096], P('dp'), parts along dimension 0
- output 2: bfloat16 [32768, 10240], P('dp', 'tp'), parts along dimension 0
- output 3: bfloat16 [32768, 10240], P('dp', 'tp'), parts along dimension 0
- output 4: bfloat16 [81920, 4096], P(('dp', 'tp')), parts along dimension 0
There are 8 independent parts. The reference program is written for one: setup_inputs(seed, part) draws one part's arguments, and reference() takes and returns one part's arrays. A program takes and returns all parts, laid end to end along the dimension named above; an argument that names none is the same for every part.
All inputs are finite; a program needn't handle non-finite values.
Results may differ from the reference program's by a relative error of at most 0.012.
Values are sent between devices in bfloat16 or wider.
A program may use at most 768 MiB of HBM per device.

```python
import jax
import jax.numpy as jnp

ROWS = 2048
D = 4096
FF = 10240


def act(gate, up):
    return jax.nn.gelu(gate) * up


def setup_inputs(seed: int = 0, part: int = 0) -> dict:
    kx, ky, ka, kb, kg, ku, kd = jax.random.split(jax.random.key(seed), 7)
    kx, ky, ka, kb = (jax.random.fold_in(k, part) for k in (kx, ky, ka, kb))
    drawn = {
        "x": jax.random.normal(kx, (ROWS, D), jnp.float32),
        "dy": jax.random.normal(ky, (ROWS, D), jnp.float32),
        "gate": jax.random.normal(ka, (ROWS, FF), jnp.float32),
        "up": jax.random.normal(kb, (ROWS, FF), jnp.float32),
        "w_gate": jax.random.normal(kg, (D, FF), jnp.float32) * D**-0.5,
        "w_up": jax.random.normal(ku, (D, FF), jnp.float32) * D**-0.5,
        "w_down": jax.random.normal(kd, (FF, D), jnp.float32) * FF**-0.5,
    }
    return {k: v.astype(jnp.bfloat16) for k, v in drawn.items()}


def reference(x, dy, gate, up, w_gate, w_up, w_down):
    hidden, back = jax.vjp(act, gate.astype(jnp.float32), up.astype(jnp.float32))
    d_hidden = jnp.dot(dy, w_down.T, preferred_element_type=jnp.float32)
    d_gate, d_up = (g.astype(jnp.bfloat16) for g in back(d_hidden))
    dx = jnp.dot(d_gate, w_gate.T, preferred_element_type=jnp.float32) + jnp.dot(d_up, w_up.T, preferred_element_type=jnp.float32)
    dw_gate = jnp.dot(x.T, d_gate, preferred_element_type=jnp.float32)
    dw_up = jnp.dot(x.T, d_up, preferred_element_type=jnp.float32)
    dw_down = jnp.dot(hidden.astype(jnp.bfloat16).T, dy, preferred_element_type=jnp.float32)
    return tuple(g.astype(jnp.bfloat16) for g in (dx, dw_gate, dw_up, dw_down))
```

```python
import functools

import jax
import jax.numpy as jnp
from jax import lax
from jax.experimental import pallas as pl
from jax.experimental.pallas import tpu as pltpu
from jax.sharding import PartitionSpec as P

MESH = pl.DeviceIdType.MESH
CUTS = 4
FB = 256
TW = 512
NT = (((1,), (1,)), ((), ()))
NN = (((1,), (0,)), ((), ()))


def act(gate, up):
    return jax.nn.gelu(gate) * up


def dot(a, b, dims):
    return lax.dot_general(a, b, dims, preferred_element_type=jnp.float32)


def kernel(
    n, x, dy, gate, up, wg, wu, wd, dx, dwg, dwu, dwd, dg, du, hid,
    wv, wdv, slot, own, dyv, guv, dblk, acc, stx, sty,
    rs_s, rs_r, ag_s, ag_r, ld, wb, wl, lo, tl, so,
):
    bf16 = jnp.bfloat16
    rows, D = x.shape
    F = gate.shape[1]
    J = CUTS
    B, W = rows // n, D // J
    H = B // 2
    NF = F // FB
    S = n - 1
    me = lax.axis_index("tp")
    nbr = (lax.rem(me + 1, n), lax.rem(me + n - 1, n))

    def block(d, t):
        return lax.rem(me + 2 * n - 1 - t, n) if d == 0 else lax.rem(me + 1 + t, n)

    def held(d, a):
        return lax.rem(me + n - a, n) if d == 0 else lax.rem(me + a, n)

    def at(b, d):
        return pl.ds(pl.multiple_of(b * B + d * H, H), H)

    def cut(j):
        return pl.ds(pl.multiple_of(j * W, W), W)

    def remote(src, dst, s, r, d):
        return pltpu.make_async_remote_copy(
            src_ref=src, dst_ref=dst, send_sem=s, recv_sem=r,
            device_id={"tp": nbr[d]}, device_id_type=MESH,
        )

    def rs_copy(d, t, j, first=False):
        src = own.at[d, j] if first else slot.at[d, t - 1, j]
        return remote(src, slot.at[d, t, j], rs_s.at[d, t, j], rs_r.at[d, t, j], d)

    def ag_copy(d, a, j, first=False):
        ref = dx.at[at(held(d, a), d), cut(j)]
        src = slot.at[d, n - 2, j] if first else ref
        return remote(src, ref, ag_s.at[d, a, j], ag_r.at[d, a, j], d)

    def mine(d, j):
        return pltpu.make_async_copy(
            slot.at[d, n - 2, j], dx.at[at(me, d), cut(j)], lo.at[d, j]
        )

    def loads(t, buf):
        out = []
        for d in range(2):
            r, v = at(block(d, t), d), pl.ds(d * H, H)
            out.append((dy.at[r, :], dyv.at[buf, v, :]))
            out.append((gate.at[r, :], guv.at[buf, 0, v, :]))
            out.append((up.at[r, :], guv.at[buf, 1, v, :]))
        return [
            pltpu.make_async_copy(s, v, ld.at[buf, i]) for i, (s, v) in enumerate(out)
        ]

    def stores(t, buf):
        out = []
        for d in range(2):
            r, v = at(block(d, t), d), pl.ds(d * H, H)
            for i, ref in enumerate((dg, du, hid)):
                out.append((dblk.at[buf, i, v, :], ref.at[r, :]))
        return [
            pltpu.make_async_copy(v, s, wb.at[buf, i]) for i, (v, s) in enumerate(out)
        ]

    def down(i):
        r = pl.ds(i * FB, FB)
        return pltpu.make_async_copy(wd.at[r, :], wdv.at[r, :], wl.at[0, i])

    def weights(j):
        r = pl.ds(j * W, W)
        return (
            pltpu.make_async_copy(wg.at[r, :], wv.at[0, r, :], wl.at[1, j]),
            pltpu.make_async_copy(wu.at[r, :], wv.at[1, r, :], wl.at[2, j]),
        )

    def gradients(buf, i):
        c = pl.ds(pl.multiple_of(i * FB, FB), FB)
        back_in = dot(dyv[buf], wdv[c, :], NT)
        g, u = guv[buf, 0, :, c].astype(jnp.float32), guv[buf, 1, :, c].astype(jnp.float32)
        h, back = jax.vjp(act, g, u)
        d_g, d_u = back(back_in)
        dblk[buf, 0, :, c] = d_g.astype(bf16)
        dblk[buf, 1, :, c] = d_u.astype(bf16)
        dblk[buf, 2, :, c] = h.astype(bf16)

    def term(buf, j):
        r = cut(j)
        return dot(dblk[buf, 0], wv[0, r, :], NT) + dot(dblk[buf, 1], wv[1, r, :], NT)

    for c in loads(0, 0):
        c.start()
    for i in range(NF):
        down(i).start()

    barrier = pltpu.get_barrier_semaphore()
    for d in range(2):
        pl.semaphore_signal(barrier, inc=1, device_id={"tp": nbr[d]}, device_id_type=MESH)

    for c in loads(0, 0):
        c.wait()
    for i in range(NF):
        down(i).wait()
        for j in range(J):
            if min(j + 1, NF - 1) == i:
                for c in weights(j):
                    c.start()
        gradients(0, i)
    for c in stores(0, 0):
        c.start()
    for c in loads(1, 1):
        c.start()
    for j in range(J):
        for c in weights(j):
            c.wait()
        part = term(0, j).astype(bf16)
        own[0, j] = part[:H]
        own[1, j] = part[H:]
        if j == 0:
            pl.semaphore_wait(barrier, 2)
        for d in range(2):
            rs_copy(d, 0, j, first=True).start()

    def step(t, carry):
        buf = lax.rem(t, 2)
        for c in loads(t, buf):
            c.wait()

        @pl.when(t >= 2)
        def _():
            for c in stores(t - 2, buf):
                c.wait()

        @pl.when(t < n - 1)
        def _():
            for c in loads(t + 1, 1 - buf):
                c.start()

        def hidden_part(i, carry):
            gradients(buf, i)
            return carry

        lax.fori_loop(0, NF, hidden_part, 0)
        for c in stores(t, buf):
            c.start()

        def piece(j, carry):
            acc[...] = term(buf, j)
            for d in range(2):
                here = slot.at[d, t - 1, j]
                remote(here, here, rs_s.at[d, t - 1, j], rs_r.at[d, t - 1, j], d).wait_recv()
                total = slot[d, t - 1, j].astype(jnp.float32) + acc[pl.ds(d * H, H), :]
                slot[d, t - 1, j] = total.astype(bf16)

            @pl.when(t < n - 1)
            def _():
                for d in range(2):
                    rs_copy(d, t, j).start()

            @pl.when(t == n - 1)
            def _():
                for d in range(2):
                    ag_copy(d, 0, j, first=True).start()
                    mine(d, j).start()

            return carry

        lax.fori_loop(0, J, piece, 0)
        return carry

    lax.fori_loop(1, n, step, 0)

    for t in (n - 2, n - 1):
        for c in stores(t, t % 2):
            c.wait()
    whole = (
        pltpu.make_async_copy(dg, wv.at[0, pl.ds(0, rows), :], wl.at[0, 0]),
        pltpu.make_async_copy(du, wv.at[0, pl.ds(rows, rows), :], wl.at[1, 0]),
        pltpu.make_async_copy(hid, wv.at[1, pl.ds(0, rows), :], wl.at[2, 0]),
    )
    NX = D // TW
    U, K = 3 * NX, S * J

    def tile_ref(s):
        return wv.at[1, pl.ds(rows, rows), pl.ds(pl.multiple_of(s * TW, TW), TW)]

    def tile(T, start):
        s = lax.rem(T, 2)

        @pl.when(T < NX)
        def _():
            c = pltpu.make_async_copy(
                x.at[:, pl.ds(pl.multiple_of(T * TW, TW), TW)], tile_ref(s), tl.at[s]
            )
            c.start() if start else c.wait()

        @pl.when((T >= NX) & (T < 2 * NX))
        def _():
            c = pltpu.make_async_copy(
                dy.at[:, pl.ds(pl.multiple_of((T - NX) * TW, TW), TW)], tile_ref(s), tl.at[s]
            )
            c.start() if start else c.wait()

    def out_x(i, g, f, p):
        r, c = pl.ds(pl.multiple_of(i * TW, TW), TW), pl.ds(pl.multiple_of(f * FB, FB), FB)
        return pltpu.make_async_copy(stx.at[p], (dwg, dwu)[g].at[r, c], so.at[0, p])

    def out_y(i, f, p):
        r, c = pl.ds(pl.multiple_of(f * FB, FB), FB), pl.ds(pl.multiple_of(i * TW, TW), TW)
        return pltpu.make_async_copy(sty.at[p], dwd.at[r, c], so.at[1, p])

    def unit_x(k):
        i, g = k // 2, lax.rem(k, 2)
        s = lax.rem(i, 2)

        @pl.when(g == 0)
        def _():
            tile(i, False)
            tile(i + 1, True)

            def turn(q, carry):
                r = pl.ds(pl.multiple_of(q * FB, FB), FB)
                wdv[pl.ds(0, TW), r] = wv[
                    1, pl.ds(pl.multiple_of(rows + q * FB, FB), FB),
                    pl.ds(pl.multiple_of(s * TW, TW), TW),
                ].T
                return carry

            lax.fori_loop(0, rows // FB, turn, 0)

        def part(f, carry):
            count = k * NF + f
            p = lax.rem(count, 2)
            res = dot(
                wdv[pl.ds(0, TW), pl.ds(0, rows)],
                wv[0, pl.ds(pl.multiple_of(g * rows, rows), rows),
                   pl.ds(pl.multiple_of(f * FB, FB), FB)],
                NN,
            ).astype(bf16)

            @pl.when(count >= 2)
            def _():
                out_x(0, 0, 0, p).wait()

            stx[p] = res
            for v in range(2):
                @pl.when(g == v)
                def _():
                    out_x(i, v, f, p).start()

            return carry

        lax.fori_loop(0, NF, part, 0)

    def unit_y(k):
        i = k - 2 * NX
        s = lax.rem(i + NX, 2)

        @pl.when(i == 0)
        def _():
            def turn(q, carry):
                r = pl.ds(pl.multiple_of(q * FB, FB), FB)
                wdv[:, pl.ds(pl.multiple_of(rows + q * FB, FB), FB)] = wv[1, r, :].T
                return carry

            lax.fori_loop(0, rows // FB, turn, 0)

        tile(i + NX, False)
        tile(i + NX + 1, True)

        def part(f, carry):
            count = i * NF + f
            p = lax.rem(count, 2)
            res = dot(
                wdv[pl.ds(pl.multiple_of(f * FB, FB), FB), pl.ds(rows, rows)],
                wv[1, pl.ds(rows, rows), pl.ds(pl.multiple_of(s * TW, TW), TW)],
                NN,
            ).astype(bf16)

            @pl.when(count >= 2)
            def _():
                out_y(0, 0, p).wait()

            sty[p] = res
            out_y(i, f, p).start()
            return carry

        lax.fori_loop(0, NF, part, 0)

    for c in whole:
        c.start()
    tile(0, True)
    for c in whole:
        c.wait()

    def tick(k, carry):
        @pl.when(k < K)
        def _():
            a = k // J + 1
            j = lax.rem(k, J)
            for d in range(2):
                ag_copy(d, a - 1, j).wait_recv()

            @pl.when(a < S)
            def _():
                for d in range(2):
                    ag_copy(d, a, j).start()

        @pl.when(k < 2 * NX)
        def _():
            unit_x(k)

        @pl.when((k >= 2 * NX) & (k < U))
        def _():
            unit_y(k)

        return carry

    lax.fori_loop(0, max(U, K), tick, 0)

    for p in range(2):
        out_x(0, 0, 0, p).wait()
        out_y(0, 0, p).wait()

    def drain(t, carry):
        def one(j, carry):
            for d in range(2):
                remote(slot.at[d, 0, j], slot.at[d, t, j], rs_s.at[d, t, j], rs_r.at[d, t, j], d).wait_send()
                ag_copy(d, t, j).wait_send()
            return carry

        return lax.fori_loop(0, J, one, carry)

    lax.fori_loop(0, n - 1, drain, 0)
    for d in range(2):
        for j in range(J):
            mine(d, j).wait()


def solution(mesh):
    n = mesh.shape["tp"]

    def step(x, dy, gate, up, w_gate, w_up, w_down):
        rows, D = x.shape
        F = gate.shape[1]
        J, B, W = CUTS, rows // n, D // CUTS
        H = B // 2
        bf16 = jnp.bfloat16
        any_ = pl.BlockSpec(memory_space=pl.ANY)
        like = lambda *s: jax.ShapeDtypeStruct(s, bf16)
        dma = pltpu.SemaphoreType.DMA
        out = pl.pallas_call(
            functools.partial(kernel, n),
            out_shape=(
                like(rows, D), like(D, F), like(D, F), like(F, D),
                like(rows, F), like(rows, F), like(rows, F),
            ),
            in_specs=[any_] * 7,
            out_specs=[any_] * 7,
            scratch_shapes=[
                pltpu.VMEM((2, D, F), bf16),
                pltpu.VMEM((F, D), bf16),
                pltpu.VMEM((2, n - 1, J, H, W), bf16),
                pltpu.VMEM((2, J, H, W), bf16),
                pltpu.VMEM((2, B, D), bf16),
                pltpu.VMEM((2, 2, B, F), bf16),
                pltpu.VMEM((2, 3, B, F), bf16),
                pltpu.VMEM((B, W), jnp.float32),
                pltpu.VMEM((2, TW, FB), bf16),
                pltpu.VMEM((2, FB, TW), bf16),
                dma((2, n - 1, J)), dma((2, n - 1, J)),
                dma((2, n - 1, J)), dma((2, n - 1, J)),
                dma((2, 6)), dma((2, 6)), dma((3, max(J, F // FB))),
                dma((2, J)), dma((2,)), dma((2, 2)),
            ],
            compiler_params=pltpu.CompilerParams(
                collective_id=0, has_side_effects=True, vmem_limit_bytes=67043328
            ),
            name="mlp_back",
        )(x, dy, gate, up, w_gate, w_up, w_down)
        return out[:4]

    tokens, columns, rows = P("dp", None), P(None, "tp"), P("tp", None)
    return jax.shard_map(
        step,
        mesh=mesh,
        in_specs=(tokens, tokens, P("dp", "tp"), P("dp", "tp"), columns, columns, rows),
        out_specs=(tokens, P("dp", "tp"), P("dp", "tp"), P(("dp", "tp"), None)),
        check_vma=False,
    )
```

```python
import functools

import jax
import jax.numpy as jnp
from jax import lax
from jax.experimental import pallas as pl
from jax.experimental.pallas import tpu as pltpu
from jax.sharding import PartitionSpec as P


MESH = pl.DeviceIdType.MESH
CUTS = 4
FB = 256
TW = 512
TAIL = 2
PARTS = 2
COPY_FLOPS = 600
NT = (((1,), (1,)), ((), ()))
TN = (((0,), (0,)), ((), ()))


def act(gate, up):
    return jax.nn.gelu(gate) * up


def dot(a, b, dims):
    return lax.dot_general(a, b, dims, preferred_element_type=jnp.float32)


def kernel(
    n, x, dy, gate, up, wg, wu, wd, dx, dwg, dwu, dwd, dg, du, hid, go00, go01, go10, go11,
    wv, wdv, slot, own, dyv, guv, dblk, acc,
    rs_s, rs_r, ag_s, ag_r, ld, wb, wl, lo, tl, so,
):
    bf16 = jnp.bfloat16
    rows, D = x.shape
    F = gate.shape[1]
    J = CUTS
    B, W = rows // n, D // J
    H = B // 2
    NF = F // FB
    S = n - 1 - TAIL
    onward = ((go00, go01), (go10, go11))
    me = lax.axis_index("tp")
    nbr = (lax.rem(me + 1, n), lax.rem(me + n - 1, n))

    def block(d, t):
        return lax.rem(me + 2 * n - 1 - t, n) if d == 0 else lax.rem(me + 1 + t, n)

    def held(d, a):
        return lax.rem(me + n - a, n) if d == 0 else lax.rem(me + a, n)

    def at(b, d):
        return pl.ds(pl.multiple_of(b * B + d * H, H), H)

    def cut(j):
        return pl.ds(pl.multiple_of(j * W, W), W)

    def remote(src, dst, s, r, d):
        return pltpu.make_async_remote_copy(
            src_ref=src, dst_ref=dst, send_sem=s, recv_sem=r,
            device_id={"tp": nbr[d]}, device_id_type=MESH,
        )

    def rs_copy(d, t, j, first=False):
        src = own.at[d, j] if first else slot.at[d, t - 1, j]
        return remote(src, slot.at[d, t, j], rs_s.at[d, t, j], rs_r.at[d, t, j], d)

    def ag_copy(d, a, j, first=False, last=None):
        ref = dx.at[at(held(d, a), d), cut(j)]
        src = slot.at[d, n - 2, j] if first else ref
        if last is not None:
            h, jh = last
            dst = onward[d][h].at[:, pl.ds(pl.multiple_of(jh * W, W), W)]
        else:
            dst = ref
        return remote(src, dst, ag_s.at[d, a, j], ag_r.at[d, a, j], d)

    def mine(d, j):
        return pltpu.make_async_copy(
            slot.at[d, n - 2, j], dx.at[at(me, d), cut(j)], lo.at[d, j]
        )

    def loads(t, buf):
        out = []
        for d in range(2):
            r, v = at(block(d, t), d), pl.ds(d * H, H)
            out.append((dy.at[r, :], dyv.at[buf, v, :]))
            out.append((gate.at[r, :], guv.at[buf, 0, v, :]))
            out.append((up.at[r, :], guv.at[buf, 1, v, :]))
        return [
            pltpu.make_async_copy(s, v, ld.at[buf, i]) for i, (s, v) in enumerate(out)
        ]

    def stores(t, buf):
        out = []
        for d in range(2):
            r, v = at(block(d, t), d), pl.ds(d * H, H)
            for i, ref in enumerate((dg, du, hid)):
                out.append((dblk.at[buf, v, pl.ds(i * F, F)], ref.at[r, :]))
        return [
            pltpu.make_async_copy(v, s, wb.at[buf, i]) for i, (v, s) in enumerate(out)
        ]

    def down(i):
        r = pl.ds(i * FB, FB)
        return pltpu.make_async_copy(wd.at[r, :], wdv.at[r, :], wl.at[0, i])

    def weights(j):
        r = pl.ds(j * W, W)
        return (
            pltpu.make_async_copy(wg.at[r, :], wv.at[r, pl.ds(0, F)], wl.at[1, j]),
            pltpu.make_async_copy(wu.at[r, :], wv.at[r, pl.ds(F, F)], wl.at[2, j]),
        )

    def gradients(buf, i):
        c = pl.ds(pl.multiple_of(i * FB, FB), FB)
        back_in = dot(dyv[buf], wdv[c, :], NT)
        g, u = guv[buf, 0, :, c].astype(jnp.float32), guv[buf, 1, :, c].astype(jnp.float32)
        h, back = jax.vjp(act, g, u)
        d_g, d_u = back(back_in)
        for k, v in enumerate((d_g, d_u, h)):
            dblk[buf, :, pl.ds(pl.multiple_of(k * F + i * FB, FB), FB)] = v.astype(bf16)

    def term(buf, j):
        return dot(dblk[buf, :, pl.ds(0, 2 * F)], wv[cut(j), :], NT)

    for c in loads(0, 0):
        c.start()
    for i in range(NF):
        down(i).start()

    barrier = pltpu.get_barrier_semaphore()
    for d in range(2):
        pl.semaphore_signal(barrier, inc=1, device_id={"tp": nbr[d]}, device_id_type=MESH)

    for c in loads(0, 0):
        c.wait()
    for i in range(NF):
        down(i).wait()
        for j in range(J):
            if min(j + 1, NF - 1) == i:
                for c in weights(j):
                    c.start()
        gradients(0, i)
    for c in stores(0, 0):
        c.start()
    for c in loads(1, 1):
        c.start()
    for j in range(J):
        for c in weights(j):
            c.wait()
        part = term(0, j).astype(bf16)
        own[0, j] = part[:H]
        own[1, j] = part[H:]
        if j == 0:
            pl.semaphore_wait(barrier, 2)
        for d in range(2):
            rs_copy(d, 0, j, first=True).start()

    def step(t, carry):
        buf = lax.rem(t, 2)
        for c in loads(t, buf):
            c.wait()

        @pl.when(t >= 2)
        def _():
            for c in stores(t - 2, buf):
                c.wait()

        @pl.when(t < n - 1)
        def _():
            for c in loads(t + 1, 1 - buf):
                c.start()

        def hidden_part(i, carry):
            gradients(buf, i)
            return carry

        lax.fori_loop(0, NF, hidden_part, 0)
        for c in stores(t, buf):
            c.start()

        def piece(j, carry):
            acc[...] = term(buf, j)
            for d in range(2):
                here = slot.at[d, t - 1, j]
                remote(here, here, rs_s.at[d, t - 1, j], rs_r.at[d, t - 1, j], d).wait_recv()
                total = slot[d, t - 1, j].astype(jnp.float32) + acc[pl.ds(d * H, H), :]
                slot[d, t - 1, j] = total.astype(bf16)

            @pl.when(t < n - 1)
            def _():
                for d in range(2):
                    rs_copy(d, t, j).start()

            @pl.when(t == n - 1)
            def _():
                for d in range(2):
                    ag_copy(d, 0, j, first=True).start()
                    mine(d, j).start()

            return carry

        lax.fori_loop(0, J, piece, 0)
        return carry

    lax.fori_loop(1, n, step, 0)

    for t in (n - 2, n - 1):
        for c in stores(t, t % 2):
            c.wait()
    top, below = pl.ds(0, rows), pl.ds(rows, rows)
    whole = (
        pltpu.make_async_copy(dg, wv.at[top, pl.ds(0, F)], wl.at[0, 0]),
        pltpu.make_async_copy(du, wv.at[top, pl.ds(F, F)], wl.at[1, 0]),
        pltpu.make_async_copy(hid, wv.at[below, pl.ds(0, F)], wl.at[2, 0]),
    )
    NX = D // TW
    U, K = 3 * NX, S * J

    def tile_cols(s):
        return pl.ds(pl.multiple_of(F + s * TW, FB), TW)

    def tile(T, start):
        s = lax.rem(T, 2)
        for ref, first in ((x, 0), (dy, NX)):
            @pl.when((T >= first) & (T < first + NX))
            def _():
                cols = pl.ds(pl.multiple_of((T - first) * TW, TW), TW)
                c = pltpu.make_async_copy(ref.at[:, cols], wv.at[below, tile_cols(s)], tl.at[s])
                c.start() if start else c.wait()

    def out_x(i, g, p):
        return pltpu.make_async_copy(
            wdv.at[pl.ds(0, TW), pl.ds(pl.multiple_of(p * F, FB), F)],
            (dwg, dwu)[g].at[pl.ds(pl.multiple_of(i * TW, TW), TW), :], so.at[0, p],
        )

    def out_y(i, p):
        return pltpu.make_async_copy(
            wdv.at[:, pl.ds(pl.multiple_of(2 * F + p * TW, TW), TW)],
            dwd.at[:, pl.ds(pl.multiple_of(i * TW, TW), TW)], so.at[1, p],
        )

    def unit_x(k):
        i, g = k // 2, lax.rem(k, 2)

        @pl.when(g == 0)
        def _():
            tile(i, False)
            tile(i + 1, True)

        @pl.when(k >= 2)
        def _():
            out_x(0, 0, g).wait()

        half = pl.ds(pl.multiple_of(g * F, FB), F)
        wdv[pl.ds(0, TW), half] = dot(
            wv[below, tile_cols(lax.rem(i, 2))], wv[top, half], TN
        ).astype(bf16)
        for v in range(2):
            @pl.when(g == v)
            def _():
                out_x(i, v, v).start()

    def unit_y(k):
        i = k - 2 * NX
        s = lax.rem(i + NX, 2)
        p = lax.rem(i, 2)

        tile(i + NX, False)
        tile(i + NX + 1, True)

        @pl.when(i >= 2)
        def _():
            out_y(0, p).wait()

        wdv[:, pl.ds(pl.multiple_of(2 * F + p * TW, TW), TW)] = dot(
            wv[below, pl.ds(0, F)], wv[below, tile_cols(s)], TN
        ).astype(bf16)
        out_y(i, p).start()

    for c in whole:
        c.start()
    tile(0, True)
    for c in whole:
        c.wait()

    def tick(k, carry):
        a = k // J + 1
        j = lax.rem(k, J)
        for d in range(2):
            ag_copy(d, a - 1, j).wait_recv()

        @pl.when(a < S - 1)
        def _():
            for d in range(2):
                ag_copy(d, a, j).start()

        for h in range(PARTS):
            jh = j - h * (J // PARTS)

            @pl.when((a == S - 1) & (jh >= 0) & (jh < J // PARTS))
            def _():
                for d in range(2):
                    ag_copy(d, a, j, last=(h, jh)).start()

        def unit(u, carry):
            @pl.when(u < 2 * NX)
            def _():
                unit_x(u)

            @pl.when(u >= 2 * NX)
            def _():
                unit_y(u)

            return carry

        @pl.when(k < spread)
        def _():
            lax.fori_loop(k * U // spread, (k + 1) * U // spread, unit, 0)

        return carry

    spread = (S - 1) * J
    lax.fori_loop(0, K, tick, 0)

    for p in range(2):
        out_x(0, p, p).wait()
        out_y(0, p).wait()

    def drain(t, carry):
        def one(j, carry):
            for d in range(2):
                remote(slot.at[d, 0, j], slot.at[d, t, j], rs_s.at[d, t, j], rs_r.at[d, t, j], d).wait_send()

            @pl.when(t < S)
            def _():
                for d in range(2):
                    ag_copy(d, t, j).wait_send()

            return carry

        return lax.fori_loop(0, J, one, carry)

    lax.fori_loop(0, n - 1, drain, 0)
    for d in range(2):
        for j in range(J):
            mine(d, j).wait()


def carry_over(moves, buf, fill, drain):
    total, depth = len(moves), buf.shape[0]
    ahead = depth // 2

    def read(i):
        return pltpu.make_async_copy(moves[i][0], buf.at[i % depth], fill.at[i % depth])

    def write(i):
        return pltpu.make_async_copy(buf.at[i % depth], moves[i][1], drain.at[i % depth])

    for i in range(total + ahead):
        if i < total:
            if i >= depth:
                write(i - depth).wait()
            read(i).start()
        if i >= ahead:
            read(i - ahead).wait()
            write(i - ahead).start()
    for i in range(max(0, total - depth), total):
        write(i).wait()


def copied(arrays, tokens=None):
    k, depth = len(arrays), 12
    rows = arrays[0].shape[0] // (32 if tokens else 16)

    def body(*refs):
        moves = []
        for src, dst in zip(refs[:k], refs[k:2 * k]):
            if tokens is None:
                starts = [i * rows for i in range(src.shape[0] // rows)]
            else:
                n, steps = tokens
                me = lax.axis_index("tp")
                B = src.shape[0] // n
                starts = []
                for a in range(steps):
                    for d in range(2):
                        b = lax.rem(me + n - a, n) if d == 0 else lax.rem(me + a, n)
                        for q in range(B // 2 // rows):
                            starts.append(pl.multiple_of(b * B + d * (B // 2) + q * rows, rows))
            for r in starts:
                moves.append((src.at[pl.ds(r, rows), :], dst.at[pl.ds(r, rows), :]))
        carry_over(moves, *refs[2 * k:])

    any_ = pl.BlockSpec(memory_space=pl.ANY)
    return pl.pallas_call(
        body,
        out_shape=tuple(jax.ShapeDtypeStruct(a.shape, a.dtype) for a in arrays),
        in_specs=[any_] * k,
        out_specs=[any_] * k,
        scratch_shapes=[
            pltpu.VMEM((depth, rows, arrays[0].shape[1]), arrays[0].dtype),
            pltpu.SemaphoreType.DMA((depth,)),
            pltpu.SemaphoreType.DMA((depth,)),
        ],
        compiler_params=pltpu.CompilerParams(vmem_limit_bytes=58 << 20),
        cost_estimate=pl.CostEstimate(
            flops=COPY_FLOPS * k * arrays[0].size, bytes_accessed=4 * k * arrays[0].size, transcendentals=0
        ),
    )(*arrays)


def place(n, steps, base, *refs):
    blocks, out, sems = refs[:-2], refs[-2], refs[-1]
    me = lax.axis_index("tp")
    H, width = blocks[0].shape
    moves = []
    for i, block in enumerate(blocks):
        step, d, h = steps[i // (2 * PARTS)], i // PARTS % 2, i % PARTS
        b = lax.rem(me + n - 1 - step, n) if d == 0 else lax.rem(me + 1 + step, n)
        for q in range(4):
            r = pl.ds(pl.multiple_of((2 * b + d) * H + q * (H // 4), H // 4), H // 4)
            src = block.at[pl.ds(q * (H // 4), H // 4), :]
            moves.append(pltpu.make_async_copy(src, out.at[r, pl.ds(h * width, width)], sems.at[i, q]))
    for c in moves:
        c.start()
    for c in moves:
        c.wait()


def placed(n, steps, base, blocks):
    any_, vmem = pl.BlockSpec(memory_space=pl.ANY), pl.BlockSpec(memory_space=pltpu.VMEM)
    return pl.pallas_call(
        functools.partial(place, n, steps),
        out_shape=jax.ShapeDtypeStruct(base.shape, base.dtype),
        in_specs=[any_, *[vmem] * len(blocks)],
        out_specs=any_,
        scratch_shapes=[pltpu.SemaphoreType.DMA((len(blocks), 4))],
        input_output_aliases={0: 0},
        compiler_params=pltpu.CompilerParams(vmem_limit_bytes=56 << 20),
        cost_estimate=pl.CostEstimate(
            flops=COPY_FLOPS * base.size // 8, bytes_accessed=base.size // 2, transcendentals=0
        ),
    )(base, *blocks)


def solution(mesh):
    n = mesh.shape["tp"]

    def step(x, dy, gate, up, w_gate, w_up, w_down):
        rows, D = x.shape
        F = gate.shape[1]
        J, B, W = CUTS, rows // n, D // CUTS
        H = B // 2
        bf16 = jnp.bfloat16
        any_ = pl.BlockSpec(memory_space=pl.ANY)
        like = lambda *s: jax.ShapeDtypeStruct(s, bf16)
        dma = pltpu.SemaphoreType.DMA
        out = pl.pallas_call(
            functools.partial(kernel, n),
            out_shape=(
                like(rows, D), like(D, F), like(D, F), like(F, D),
                like(rows, F), like(rows, F), like(rows, F),
                *[like(H, D // PARTS)] * (2 * PARTS),
            ),
            in_specs=[any_] * 7,
            out_specs=[any_] * (7 + 2 * PARTS),
            scratch_shapes=[
                pltpu.VMEM((D, 2 * F), bf16),
                pltpu.VMEM((F, D), bf16),
                pltpu.VMEM((2, n - 1, J, H, W), bf16),
                pltpu.VMEM((2, J, H, W), bf16),
                pltpu.VMEM((2, B, D), bf16),
                pltpu.VMEM((2, 2, B, F), bf16),
                pltpu.VMEM((2, B, 3 * F), bf16),
                pltpu.VMEM((B, W), jnp.float32),
                dma((2, n - 1, J)), dma((2, n - 1, J)),
                dma((2, n - 1, J)), dma((2, n - 1, J)),
                dma((2, 6)), dma((2, 6)), dma((3, max(J, F // FB))),
                dma((2, J)), dma((2,)), dma((2, 2)),
            ],
            compiler_params=pltpu.CompilerParams(
                collective_id=0, has_side_effects=True, vmem_limit_bytes=67043328
            ),
            name="mlp_back",
        )(x, dy, gate, up, w_gate, w_up, w_down)

        def hop(d, a):
            by = 1 if d == 0 else n - 1
            return lax.ppermute(a, "tp", [(q, (q + by) % n) for q in range(n)])

        S = n - 1 - TAIL
        dwg, dwu = copied(out[1:3])
        (dwd,) = copied(out[3:4])
        (dx,) = copied(out[:1], (n, S))
        onward = {(d, h): out[7 + d * PARTS + h] for h in range(PARTS) for d in range(2)}
        arrived = [onward]
        for _ in range(TAIL):
            onward = {(d, h): hop(d, a) for (d, h), a in onward.items()}
            arrived.append(onward)
        arrived = [[got[d, h] for d in range(2) for h in range(PARTS)] for got in arrived]
        dx = placed(n, (S - 1, S), dx, arrived[0] + arrived[1])
        for k in range(1, TAIL):
            dx = placed(n, (S + k,), dx, arrived[k + 1])
        return dx, dwg, dwu, dwd

    tokens, columns, rows = P("dp", None), P(None, "tp"), P("tp", None)
    return jax.shard_map(
        step,
        mesh=mesh,
        in_specs=(tokens, tokens, P("dp", "tp"), P("dp", "tp"), columns, columns, rows),
        out_specs=(tokens, P("dp", "tp"), P("dp", "tp"), P(("dp", "tp"), None)),
        check_vma=False,
    )
```

```python
import functools

import jax
import jax.numpy as jnp
from jax import lax
from jax.experimental import pallas as pl
from jax.experimental.pallas import tpu as pltpu
from jax.sharding import PartitionSpec as P


MESH = pl.DeviceIdType.MESH
CUTS = 4
FB = 256
TW = 512
TAIL = 2
PARTS = 2
COPY_FLOPS = 600
NT = (((1,), (1,)), ((), ()))
TN = (((0,), (0,)), ((), ()))


def act(gate, up):
    return jax.nn.gelu(gate) * up


def dot(a, b, dims):
    return lax.dot_general(a, b, dims, preferred_element_type=jnp.float32)


def kernel(
    n, x, dy, gate, up, wg, wu, wd, dx, dwg, dwu, dwd, dg, du, hid, go00, go01, go10, go11,
    wv, wdv, slot, own, dyv, guv, dblk, acc,
    rs_s, rs_r, ag_s, ag_r, ld, wb, wl, lo, tl, so,
):
    bf16 = jnp.bfloat16
    rows, D = x.shape
    F = gate.shape[1]
    J = CUTS
    B, W = rows // n, D // J
    H = B // 2
    NF = F // FB
    S = n - 1 - TAIL
    onward = ((go00, go01), (go10, go11))
    me = lax.axis_index("tp")
    nbr = (lax.rem(me + 1, n), lax.rem(me + n - 1, n))

    def block(d, t):
        return lax.rem(me + 2 * n - 1 - t, n) if d == 0 else lax.rem(me + 1 + t, n)

    def held(d, a):
        return lax.rem(me + n - a, n) if d == 0 else lax.rem(me + a, n)

    def at(b, d):
        return pl.ds(pl.multiple_of(b * B + d * H, H), H)

    def cut(j):
        return pl.ds(pl.multiple_of(j * W, W), W)

    def remote(src, dst, s, r, d):
        return pltpu.make_async_remote_copy(
            src_ref=src, dst_ref=dst, send_sem=s, recv_sem=r,
            device_id={"tp": nbr[d]}, device_id_type=MESH,
        )

    def rs_copy(d, t, j, first=False):
        src = own.at[d, j] if first else slot.at[d, t - 1, j]
        return remote(src, slot.at[d, t, j], rs_s.at[d, t, j], rs_r.at[d, t, j], d)

    def ag_copy(d, a, j, first=False, last=None):
        ref = dx.at[at(held(d, a), d), cut(j)]
        src = slot.at[d, n - 2, j] if first else ref
        if last is not None:
            h, jh = last
            dst = onward[d][h].at[:, pl.ds(pl.multiple_of(jh * W, W), W)]
        else:
            dst = ref
        return remote(src, dst, ag_s.at[d, a, j], ag_r.at[d, a, j], d)

    def mine(d, j):
        return pltpu.make_async_copy(
            slot.at[d, n - 2, j], dx.at[at(me, d), cut(j)], lo.at[d, j]
        )

    def loads(t, buf):
        out = []
        for d in range(2):
            r, v = at(block(d, t), d), pl.ds(d * H, H)
            out.append((dy.at[r, :], dyv.at[buf, v, :]))
            out.append((gate.at[r, :], guv.at[buf, 0, v, :]))
            out.append((up.at[r, :], guv.at[buf, 1, v, :]))
        return [
            pltpu.make_async_copy(s, v, ld.at[buf, i]) for i, (s, v) in enumerate(out)
        ]

    def stores(t, buf):
        out = []
        for d in range(2):
            r, v = at(block(d, t), d), pl.ds(d * H, H)
            for i, ref in enumerate((dg, du, hid)):
                out.append((dblk.at[buf, v, pl.ds(i * F, F)], ref.at[r, :]))
        return [
            pltpu.make_async_copy(v, s, wb.at[buf, i]) for i, (v, s) in enumerate(out)
        ]

    def down(i):
        r = pl.ds(i * FB, FB)
        return pltpu.make_async_copy(wd.at[r, :], wdv.at[r, :], wl.at[0, i])

    def weights(j):
        r = pl.ds(j * W, W)
        return (
            pltpu.make_async_copy(wg.at[r, :], wv.at[r, pl.ds(0, F)], wl.at[1, j]),
            pltpu.make_async_copy(wu.at[r, :], wv.at[r, pl.ds(F, F)], wl.at[2, j]),
        )

    def gradients(buf, i):
        c = pl.ds(pl.multiple_of(i * FB, FB), FB)
        back_in = dot(dyv[buf], wdv[c, :], NT)
        g, u = guv[buf, 0, :, c].astype(jnp.float32), guv[buf, 1, :, c].astype(jnp.float32)
        h, back = jax.vjp(act, g, u)
        d_g, d_u = back(back_in)
        for k, v in enumerate((d_g, d_u, h)):
            dblk[buf, :, pl.ds(pl.multiple_of(k * F + i * FB, FB), FB)] = v.astype(bf16)

    def term(buf, j):
        return dot(dblk[buf, :, pl.ds(0, 2 * F)], wv[cut(j), :], NT)

    for c in loads(0, 0):
        c.start()
    for i in range(NF):
        down(i).start()

    barrier = pltpu.get_barrier_semaphore()
    for d in range(2):
        pl.semaphore_signal(barrier, inc=1, device_id={"tp": nbr[d]}, device_id_type=MESH)

    for c in loads(0, 0):
        c.wait()
    for i in range(NF):
        down(i).wait()
        for j in range(J):
            if min(j + 1, NF - 1) == i:
                for c in weights(j):
                    c.start()
        gradients(0, i)
    for c in stores(0, 0):
        c.start()
    for c in loads(1, 1):
        c.start()
    for j in range(J):
        for c in weights(j):
            c.wait()
        part = term(0, j).astype(bf16)
        own[0, j] = part[:H]
        own[1, j] = part[H:]
        if j == 0:
            pl.semaphore_wait(barrier, 2)
        for d in range(2):
            rs_copy(d, 0, j, first=True).start()

    def step(t, carry):
        buf = lax.rem(t, 2)
        for c in loads(t, buf):
            c.wait()

        @pl.when(t >= 2)
        def _():
            for c in stores(t - 2, buf):
                c.wait()

        @pl.when(t < n - 1)
        def _():
            for c in loads(t + 1, 1 - buf):
                c.start()

        def hidden_part(i, carry):
            gradients(buf, i)
            return carry

        lax.fori_loop(0, NF, hidden_part, 0)
        for c in stores(t, buf):
            c.start()

        def piece(j, carry):
            acc[...] = term(buf, j)
            for d in range(2):
                here = slot.at[d, t - 1, j]
                remote(here, here, rs_s.at[d, t - 1, j], rs_r.at[d, t - 1, j], d).wait_recv()
                total = slot[d, t - 1, j].astype(jnp.float32) + acc[pl.ds(d * H, H), :]
                slot[d, t - 1, j] = total.astype(bf16)

            @pl.when(t < n - 1)
            def _():
                for d in range(2):
                    rs_copy(d, t, j).start()

            @pl.when(t == n - 1)
            def _():
                for d in range(2):
                    ag_copy(d, 0, j, first=True).start()
                    mine(d, j).start()

            return carry

        lax.fori_loop(0, J, piece, 0)
        return carry

    lax.fori_loop(1, n, step, 0)

    for t in (n - 2, n - 1):
        for c in stores(t, t % 2):
            c.wait()
    top, below = pl.ds(0, rows), pl.ds(rows, rows)
    whole = (
        pltpu.make_async_copy(dg, wv.at[top, pl.ds(0, F)], wl.at[0, 0]),
        pltpu.make_async_copy(du, wv.at[top, pl.ds(F, F)], wl.at[1, 0]),
        pltpu.make_async_copy(hid, wv.at[below, pl.ds(0, F)], wl.at[2, 0]),
    )
    NX = D // TW
    U, K = 3 * NX, S * J

    def tile_cols(s):
        return pl.ds(pl.multiple_of(F + s * TW, FB), TW)

    def tile(T, start):
        s = lax.rem(T, 2)
        for ref, first in ((x, 0), (dy, NX)):
            @pl.when((T >= first) & (T < first + NX))
            def _():
                cols = pl.ds(pl.multiple_of((T - first) * TW, TW), TW)
                c = pltpu.make_async_copy(ref.at[:, cols], wv.at[below, tile_cols(s)], tl.at[s])
                c.start() if start else c.wait()

    def out_x(i, g, p):
        return pltpu.make_async_copy(
            wdv.at[pl.ds(0, TW), pl.ds(pl.multiple_of(p * F, FB), F)],
            (dwg, dwu)[g].at[pl.ds(pl.multiple_of(i * TW, TW), TW), :], so.at[0, p],
        )

    def out_y(i, p):
        return pltpu.make_async_copy(
            wdv.at[:, pl.ds(pl.multiple_of(2 * F + p * TW, TW), TW)],
            dwd.at[:, pl.ds(pl.multiple_of(i * TW, TW), TW)], so.at[1, p],
        )

    def unit_x(k):
        i, g = k // 2, lax.rem(k, 2)

        @pl.when(g == 0)
        def _():
            tile(i, False)
            tile(i + 1, True)

        @pl.when(k >= 2)
        def _():
            out_x(0, 0, g).wait()

        half = pl.ds(pl.multiple_of(g * F, FB), F)
        wdv[pl.ds(0, TW), half] = dot(
            wv[below, tile_cols(lax.rem(i, 2))], wv[top, half], TN
        ).astype(bf16)
        for v in range(2):
            @pl.when(g == v)
            def _():
                out_x(i, v, v).start()

    def unit_y(k):
        i = k - 2 * NX
        s = lax.rem(i + NX, 2)
        p = lax.rem(i, 2)

        tile(i + NX, False)
        tile(i + NX + 1, True)

        @pl.when(i >= 2)
        def _():
            out_y(0, p).wait()

        wdv[:, pl.ds(pl.multiple_of(2 * F + p * TW, TW), TW)] = dot(
            wv[below, pl.ds(0, F)], wv[below, tile_cols(s)], TN
        ).astype(bf16)
        out_y(i, p).start()

    for c in whole:
        c.start()
    tile(0, True)

    def tick(k, carry):
        a = k // J + 1
        j = lax.rem(k, J)
        for d in range(2):
            ag_copy(d, a - 1, j).wait_recv()

        @pl.when(a < S - 1)
        def _():
            for d in range(2):
                ag_copy(d, a, j).start()

        for h in range(PARTS):
            jh = j - h * (J // PARTS)

            @pl.when((a == S - 1) & (jh >= 0) & (jh < J // PARTS))
            def _():
                for d in range(2):
                    ag_copy(d, a, j, last=(h, jh)).start()

        def unit(u, carry):
            @pl.when(u < 2 * NX)
            def _():
                unit_x(u)

            @pl.when(u >= 2 * NX)
            def _():
                unit_y(u)

            return carry

        @pl.when(k == 0)
        def _():
            for c in whole:
                c.wait()

        @pl.when(k < spread)
        def _():
            lax.fori_loop(k * U // spread, (k + 1) * U // spread, unit, 0)

        return carry

    spread = S * J - 2
    lax.fori_loop(0, K, tick, 0)

    for p in range(2):
        out_x(0, p, p).wait()
        out_y(0, p).wait()

    def drain(t, carry):
        def one(j, carry):
            for d in range(2):
                remote(slot.at[d, 0, j], slot.at[d, t, j], rs_s.at[d, t, j], rs_r.at[d, t, j], d).wait_send()

            @pl.when(t < S)
            def _():
                for d in range(2):
                    ag_copy(d, t, j).wait_send()

            return carry

        return lax.fori_loop(0, J, one, carry)

    lax.fori_loop(0, n - 1, drain, 0)
    for d in range(2):
        for j in range(J):
            mine(d, j).wait()


def carry_over(moves, buf, fill, drain):
    total, depth = len(moves), buf.shape[0]
    ahead = depth // 2

    def read(i):
        return pltpu.make_async_copy(moves[i][0], buf.at[i % depth], fill.at[i % depth])

    def write(i):
        return pltpu.make_async_copy(buf.at[i % depth], moves[i][1], drain.at[i % depth])

    for i in range(total + ahead):
        if i < total:
            if i >= depth:
                write(i - depth).wait()
            read(i).start()
        if i >= ahead:
            read(i - ahead).wait()
            write(i - ahead).start()
    for i in range(max(0, total - depth), total):
        write(i).wait()


def copied(arrays, tokens=None):
    k, depth = len(arrays), 12
    rows = arrays[0].shape[0] // (32 if tokens else 16)

    def body(*refs):
        moves = []
        for src, dst in zip(refs[:k], refs[k:2 * k]):
            if tokens is None:
                starts = [i * rows for i in range(src.shape[0] // rows)]
            else:
                n, steps = tokens
                me = lax.axis_index("tp")
                B = src.shape[0] // n
                starts = []
                for a in range(steps):
                    for d in range(2):
                        b = lax.rem(me + n - a, n) if d == 0 else lax.rem(me + a, n)
                        for q in range(B // 2 // rows):
                            starts.append(pl.multiple_of(b * B + d * (B // 2) + q * rows, rows))
            for r in starts:
                moves.append((src.at[pl.ds(r, rows), :], dst.at[pl.ds(r, rows), :]))
        carry_over(moves, *refs[2 * k:])

    hbm = pl.BlockSpec(memory_space=pltpu.HBM)
    return pl.pallas_call(
        body,
        out_shape=tuple(jax.ShapeDtypeStruct(a.shape, a.dtype) for a in arrays),
        in_specs=[hbm] * k,
        out_specs=[hbm] * k,
        scratch_shapes=[
            pltpu.VMEM((depth, rows, arrays[0].shape[1]), arrays[0].dtype),
            pltpu.SemaphoreType.DMA((depth,)),
            pltpu.SemaphoreType.DMA((depth,)),
        ],
        compiler_params=pltpu.CompilerParams(vmem_limit_bytes=56 << 20),
        cost_estimate=pl.CostEstimate(
            flops=COPY_FLOPS * k * arrays[0].size, bytes_accessed=4 * k * arrays[0].size, transcendentals=0
        ),
    )(*arrays)


def place(n, whence, base, *refs):
    blocks, out, sems = refs[:-2], refs[-2], refs[-1]
    me = lax.axis_index("tp")
    H, width = blocks[0].shape
    moves = []
    for i, block in enumerate(blocks):
        step, d, h = whence[i]
        b = lax.rem(me + n - 1 - step, n) if d == 0 else lax.rem(me + 1 + step, n)
        for q in range(4):
            r = pl.ds(pl.multiple_of((2 * b + d) * H + q * (H // 4), H // 4), H // 4)
            src = block.at[pl.ds(q * (H // 4), H // 4), :]
            moves.append(pltpu.make_async_copy(src, out.at[r, pl.ds(h * width, width)], sems.at[i, q]))
    for c in moves:
        c.start()
    for c in moves:
        c.wait()


def placed(n, base, arrived):
    hbm, vmem = pl.BlockSpec(memory_space=pltpu.HBM), pl.BlockSpec(memory_space=pltpu.VMEM)
    whence, blocks = list(arrived), list(arrived.values())
    return pl.pallas_call(
        functools.partial(place, n, whence),
        out_shape=jax.ShapeDtypeStruct(base.shape, base.dtype),
        in_specs=[hbm, *[vmem] * len(blocks)],
        out_specs=hbm,
        scratch_shapes=[pltpu.SemaphoreType.DMA((len(blocks), 4))],
        input_output_aliases={0: 0},
        compiler_params=pltpu.CompilerParams(vmem_limit_bytes=16 << 20),
        cost_estimate=pl.CostEstimate(
            flops=COPY_FLOPS * base.size // 8, bytes_accessed=base.size // 2, transcendentals=0
        ),
    )(base, *blocks)


def solution(mesh):
    n = mesh.shape["tp"]

    def step(x, dy, gate, up, w_gate, w_up, w_down):
        rows, D = x.shape
        F = gate.shape[1]
        J, B, W = CUTS, rows // n, D // CUTS
        H = B // 2
        bf16 = jnp.bfloat16
        any_ = pl.BlockSpec(memory_space=pl.ANY)
        like = lambda *s: jax.ShapeDtypeStruct(s, bf16)
        dma = pltpu.SemaphoreType.DMA
        out = pl.pallas_call(
            functools.partial(kernel, n),
            out_shape=(
                like(rows, D), like(D, F), like(D, F), like(F, D),
                like(rows, F), like(rows, F), like(rows, F),
                *[like(H, D // PARTS)] * (2 * PARTS),
            ),
            in_specs=[any_] * 7,
            out_specs=[any_] * (7 + 2 * PARTS),
            scratch_shapes=[
                pltpu.VMEM((D, 2 * F), bf16),
                pltpu.VMEM((F, D), bf16),
                pltpu.VMEM((2, n - 1, J, H, W), bf16),
                pltpu.VMEM((2, J, H, W), bf16),
                pltpu.VMEM((2, B, D), bf16),
                pltpu.VMEM((2, 2, B, F), bf16),
                pltpu.VMEM((2, B, 3 * F), bf16),
                pltpu.VMEM((B, W), jnp.float32),
                dma((2, n - 1, J)), dma((2, n - 1, J)),
                dma((2, n - 1, J)), dma((2, n - 1, J)),
                dma((2, 6)), dma((2, 6)), dma((3, max(J, F // FB))),
                dma((2, J)), dma((2,)), dma((2, 2)),
            ],
            compiler_params=pltpu.CompilerParams(
                collective_id=0, has_side_effects=True, vmem_limit_bytes=67043328
            ),
            name="mlp_back",
        )(x, dy, gate, up, w_gate, w_up, w_down)

        def hop(d, a):
            by = 1 if d == 0 else n - 1
            return lax.ppermute(a, "tp", [(q, (q + by) % n) for q in range(n)])

        S = n - 1 - TAIL
        dwg, dwu = copied(out[1:3])
        (dwd,) = copied(out[3:4])
        (dx,) = copied(out[:1], (n, S))
        onward = {(d, h): out[7 + d * PARTS + h] for h in range(PARTS) for d in range(2)}
        arrived = {(S - 1, *i): a for i, a in onward.items()}
        for k in range(TAIL):
            onward = {(d, h): hop(d, a) for (d, h), a in onward.items()}
            arrived |= {(S + k, *i): a for i, a in onward.items()}
        for now in (
            lambda step, h: step < n - 2,
            *[lambda step, h, part=part: step == n - 2 and h == part for part in range(PARTS)],
        ):
            dx = placed(n, dx, {i: a for i, a in arrived.items() if now(i[0], i[2])})
        return dx, dwg, dwu, dwd

    tokens, columns, rows = P("dp", None), P(None, "tp"), P("tp", None)
    return jax.shard_map(
        step,
        mesh=mesh,
        in_specs=(tokens, tokens, P("dp", "tp"), P("dp", "tp"), columns, columns, rows),
        out_specs=(tokens, P("dp", "tp"), P("dp", "tp"), P(("dp", "tp"), None)),
        check_vma=False,
    )
```
